32 devices in a mesh: groups: 2 (over x), expert: 16 (over z, y, core).
Axes of the slice: x: 2, y: 2, z: 4, core: 2. Of those that a mesh axis runs over, the one named last changes fastest.
Arguments:
- tokens: bfloat16 [4096, 4096], P(('groups', 'expert')), parts along dimension 0, may hold values from -6 to 6
- router_weight: bfloat16 [4096, 128], replicated, may hold values from -0.078125 to 0.078125
- expert_ids: int32 [4096, 8], P(('groups', 'expert')), parts along dimension 0, may hold values from 0 to 127, all different within a row; in each aligned block of 128 rows (0 to 127, 128 to 255, ...) at most 9 rows name the same one
Outputs:
- expert_rows: bfloat16 [128, 288, 4096], P('expert', 'groups'), parts along dimension 1
- balance_loss: float32 [2], P('groups'), parts along dimension 0
The draws below stay inside these ranges and needn't reach their ends.
There are 2 independent parts, one for each index of `groups`. The reference program is written for one: setup_inputs(seed, part) draws one part's arguments, and reference() takes and returns one part's arrays. A program takes and returns all parts, laid end to end along the dimension named above; an argument that names none is the same for every part. Nothing has to cross between parts.
Inputs may be any that keep to these rules, and one draw needn't show every extreme that they name: `expert_ids`: each row names 8 different experts; among the rows of one device no expert is named more than 9 times, a bound that some block reaches.
All inputs are finite; a program needn't handle non-finite values.
Results may differ from the reference program's by a relative error of at most 0.0012.
Values may be sent and summed in bfloat16 or wider, within the bound.
A program may use at most 128 MiB of HBM per device.

```python
import math
import jax
import jax.numpy as jnp
import numpy as np

D = 4096
EXPERTS = 128
TOP_K = 8
TOK_DEV = 128
CAP = 9
TOKENS = 2048
SLOTS = 144
N_EXPERT = 16


def pattern_signs(count):
    index = jnp.arange(count, dtype=jnp.int32)
    parity = jnp.zeros((count,), jnp.int32)
    for bit_place in range(20):
        parity = parity + jnp.bitwise_and(jnp.right_shift(index, bit_place), 1)
    return 1.0 - 2.0 * jnp.bitwise_and(parity, 1).astype(jnp.float32)


def draw_router_weight(key, part):
    first = jax.random.fold_in(key, 11)
    second = jax.random.fold_in(key, 12)
    noise = jnp.clip(jax.random.normal(first, (D, EXPERTS), jnp.float32), -4.0, 4.0)
    amplitude = jax.random.uniform(second, (EXPERTS,), jnp.float32, 0.3, 1.0)
    combined = (noise + amplitude[None, :] * pattern_signs(D)[:, None]) * D ** (-0.5)
    return combined.astype(jnp.bfloat16)


def draw_tokens(key, part):
    first = jax.random.fold_in(key, 21)
    second = jax.random.fold_in(key, 22)
    third = jax.random.fold_in(key, 23)
    rise = jnp.arange(TOKENS, dtype=jnp.float32) / max(TOKENS - 1, 1)
    base = jnp.clip(jax.random.normal(first, (TOKENS, D), jnp.float32), -6.0, 6.0)
    share = 1.0 / 32.0 * jnp.exp(rise * jnp.log(8.0))
    chosen_rows = jax.random.uniform(second, (TOKENS,), jnp.float32) < share
    strength = jax.random.randint(third, (TOKENS,), 2, 7).astype(jnp.float32)
    planted = strength[:, None] * pattern_signs(D)[None, :]
    return jnp.where(chosen_rows[:, None], planted, base).astype(jnp.bfloat16)


def deal_out(rng, own, number, rows, number_of, top, reach, lean):
    order = jax.random.permutation(rng, number_of)
    crowded, usual = load_shares(number_of, rows * top, reach, lean, True), load_shares(number_of, rows * top, reach, lean, False)
    places = jnp.arange(number_of)

    def named(tallies, offset_by):
        used = int((tallies > 0).sum())
        fixed = max(1, used // 4)
        moved = fixed + (places - fixed + offset_by * (used - fixed)) % max(1, number_of - fixed)
        return jnp.zeros((number_of,), jnp.int32).at[order[jnp.where(places < fixed, places, moved)]].set(jnp.asarray(tallies, jnp.int32))

    tallies = jnp.where(number % 4 == 0, named(crowded, number // 4), named(usual, number - number // 4 - 1))
    mixed = jax.random.permutation(jax.random.fold_in(own, 3), number_of)
    giver, receiver = mixed[0:number_of // 2 * 2:2], mixed[1:number_of // 2 * 2:2]
    slack = jnp.minimum(tallies[giver] - 1, reach - tallies[receiver]) // 2
    slack = jnp.where((giver == order[0]) | (receiver == order[0]) | (tallies[receiver] == 0), 0, jnp.maximum(slack, 0))
    moved = jax.random.randint(jax.random.fold_in(own, 4), (number_of // 2,), 0, 1 << 20) % (slack + 1)
    tallies = tallies.at[giver].add(-moved).at[receiver].add(moved)
    members = jnp.searchsorted(jnp.cumsum(tallies), jnp.arange(rows * top), side="right").astype(jnp.int32)
    listing = members.reshape(top, rows).T
    listing = listing[jax.random.permutation(jax.random.fold_in(own, 1), rows)]
    offset_by = jax.random.randint(jax.random.fold_in(own, 2), (rows, 1), 0, top)
    return jnp.take_along_axis(listing, (jnp.arange(top)[None, :] + offset_by) % top, axis=1)


def load_shares(count, total, bound, skew, full):
    weights = [(1 << 20) // math.isqrt(standing ** skew) + 1 for standing in range(1, count + 1)]
    largest = bound if full else min(bound, max(-(-total // count), total * weights[0] // sum(weights)))
    least = 1 if total - largest >= count - 1 else 0
    counts, surplus = [largest] + [least] * (count - 1), total - largest - least * (count - 1)
    while surplus > 0:
        candidates = [i for i in range(1, count) if counts[i] < largest] or [i for i in range(1, count) if counts[i] < bound]
        mass, left = sum([weights[i] for i in candidates]), surplus
        for i in candidates:
            more = min(bound - counts[i], max(1, left * weights[i] // mass), surplus)
            counts[i] = counts[i] + more
            surplus = surplus - more
    return np.array(counts)


def setup_inputs(seed: int = 0, part: int = 0) -> dict:
    keys = jax.random.split(jax.random.key(seed), 4)
    part_splits = jax.random.split(jax.random.fold_in(keys[3], part), 4)
    tokens = draw_tokens(jax.random.fold_in(jax.random.fold_in(keys[3], part), 71), part)
    router_weight = draw_router_weight(jax.random.fold_in(keys[3], 71), part)
    expert_ids_keys = jax.random.split(jax.random.fold_in(part_splits[2], 1), TOKENS // TOK_DEV)
    expert_ids_turns = jax.random.permutation(jax.random.fold_in(part_splits[2], 3), TOKENS // TOK_DEV)
    expert_ids = jax.vmap(lambda own, number: deal_out(jax.random.fold_in(part_splits[2], 2), own, number, TOK_DEV, EXPERTS, TOP_K, CAP, 2))(expert_ids_keys, expert_ids_turns).reshape((TOKENS, TOP_K))
    return dict(tokens=tokens, router_weight=router_weight, expert_ids=expert_ids)


def reference(tokens, router_weight, expert_ids):
    logits = jnp.dot(tokens, router_weight, preferred_element_type=jnp.float32)
    probability = jax.nn.softmax(logits, axis=-1)
    chosen = jnp.take_along_axis(logits, expert_ids, axis=1)
    gates = jax.nn.softmax(chosen, axis=1)
    onehot = jnp.sum((expert_ids[:, :, None] == jnp.arange(EXPERTS, dtype=jnp.int32)[None, None, :]).astype(jnp.int32), axis=1).astype(jnp.int32)
    blocks = onehot.reshape(N_EXPERT, TOK_DEV, EXPERTS)
    before = (jnp.cumsum(blocks, axis=1) - blocks).astype(jnp.int32).reshape(TOKENS, EXPERTS)
    slot_rank = jnp.take_along_axis(before, expert_ids, axis=1).astype(jnp.int32)
    owner_index = (jnp.arange(TOKENS, dtype=jnp.int32) // TOK_DEV)[:, None]
    position = (owner_index * CAP + slot_rank).astype(jnp.int32)
    widened = tokens.astype(jnp.float32)
    expert_rows = jnp.zeros((EXPERTS, SLOTS, D), jnp.bfloat16)
    for column in range(TOP_K):
        gated = (gates[:, column:column + 1] * widened).astype(jnp.bfloat16)
        expert_rows = expert_rows.at[expert_ids[:, column], position[:, column]].set(gated)
    expert_load = jnp.sum(onehot, axis=0).astype(jnp.float32)
    expert_mass = jnp.sum(probability, axis=0)
    token_total = jnp.float32(TOKENS)
    balance_loss = EXPERTS * jnp.sum(expert_load * expert_mass) / (token_total * token_total * TOP_K)
    return expert_rows, balance_loss.reshape(1)
```

```python
import functools

import jax
import jax.numpy as jnp
from jax import lax
from jax.experimental import pallas as pl
from jax.experimental.pallas import tpu as pltpu
from jax.sharding import PartitionSpec as P

EXPERTS = 128
TOP_K = 8
CAP = 9
LANES = 128
LEFT, RIGHT, ACROSS, SIBLING = range(4)
PIECES = 3


def column_chunks(width):
    tiles = width // LANES
    side = max(1, tiles * 5 // 32)
    main = tiles - side
    edges = [main * i // PIECES for i in range(PIECES + 1)] + [tiles]
    return [(a * LANES, (b - a) * LANES) for a, b in zip(edges[:-1], edges[1:])]


def gather_kernel(n, x_ref, w_ref, ids_ref, buf, rmsg, msg, ssem, rsem, smsem, rmsem, lsem):
    depth = n // 4
    me = lax.axis_index("expert")
    group = lax.axis_index("groups")
    z, y, c = me // 4, (me // 2) % 2, me % 2
    yp, cp = 1 - y, 1 - c
    chunks = column_chunks(x_ref.shape[1])
    last = len(chunks) - 1

    def at(zz, yy, cc):
        return zz * 4 + yy * 2 + cc

    def ident(target):
        return (group, target)

    barrier = pltpu.get_barrier_semaphore()
    for o in range(1, n):
        pl.semaphore_signal(
            barrier, inc=1, device_id=ident((me + o) % n), device_id_type=pl.DeviceIdType.MESH
        )
    pl.semaphore_wait(barrier, n - 1)

    where = {
        LEFT: at(z - 1, y, c),
        RIGHT: at(z + 1, y, c),
        ACROSS: at(z, yp, c),
        SIBLING: at(z, y, cp),
    }
    exists = {LEFT: z > 0, RIGHT: z < depth - 1, ACROSS: None, SIBLING: None}
    sent = []

    def copy_of(src, k, way, own=False):
        start, width = chunks[k]
        cols = pl.ds(start, width)
        source = x_ref.at[:, cols] if own else buf.at[src, :, cols]
        return pltpu.make_async_remote_copy(
            src_ref=source,
            dst_ref=buf.at[src, :, cols],
            send_sem=ssem.at[src, k, way],
            recv_sem=rsem.at[src, k],
            device_id=ident(where[way]),
            device_id_type=pl.DeviceIdType.MESH,
        )

    def guarded(cond, fn):
        if cond is None:
            fn()
        else:
            pl.when(cond)(fn)

    def send(src, k, way, own=False, held=None):
        copy = copy_of(src, k, way, own)
        guarded(exists[way], copy.start)
        sent.append((held, way, src, k, own))

    def arrived(src, k):
        copy_of(src, k, SIBLING).wait_recv()

    for k in range(last):
        for way in (LEFT, RIGHT, ACROSS, SIBLING):
            send(me, k, way, own=True)
    send(me, last, ACROSS, own=True)
    send(me, last, SIBLING, own=True)
    keep = pltpu.make_async_copy(x_ref, buf.at[me], lsem)
    keep.start()

    rows = x_ref.shape[0]
    logits = jnp.dot(x_ref[...], w_ref[...], preferred_element_type=jnp.float32)
    ids = ids_ref[...]
    lane = lax.broadcasted_iota(jnp.int32, (rows, EXPERTS), 1)
    named = ids[:, 0:1] == lane
    for k in range(1, TOP_K):
        named = jnp.logical_or(named, ids[:, k : k + 1] == lane)
    mask = jnp.where(named, 1.0, 0.0)
    raised = jnp.exp(logits - jnp.max(logits, axis=1, keepdims=True))
    probability = raised / jnp.sum(raised, axis=1, keepdims=True)
    chosen = jnp.where(named, logits, -1e30)
    picked = jnp.where(named, jnp.exp(chosen - jnp.max(chosen, axis=1, keepdims=True)), 0.0)
    gates = picked / jnp.sum(picked, axis=1, keepdims=True)
    r = lax.broadcasted_iota(jnp.int32, (rows, rows), 0)
    q = lax.broadcasted_iota(jnp.int32, (rows, rows), 1)
    lower = jnp.where(q < r, 1.0, 0.0).astype(jnp.bfloat16)
    before = jnp.dot(lower, mask.astype(jnp.bfloat16), preferred_element_type=jnp.float32)
    rank = jnp.where(named, before, -1.0)
    mine = EXPERTS // n
    msg[:, 0] = gates.T.reshape(n, mine, rows)
    msg[:, 1] = rank.T.reshape(n, mine, rows)
    stat_row = lax.broadcasted_iota(jnp.int32, (mine, EXPERTS), 0)
    load = jnp.sum(mask, axis=0, keepdims=True)
    mass = jnp.sum(probability, axis=0, keepdims=True)
    stats = jnp.where(stat_row == 0, load, jnp.where(stat_row == 1, mass, 0.0))
    msg[:, 2] = jnp.broadcast_to(stats[None], (n, mine, EXPERTS))
    rmsg[me] = msg[me]

    def note_of(target, source):
        return pltpu.make_async_remote_copy(
            src_ref=msg.at[target],
            dst_ref=rmsg.at[source],
            send_sem=smsem.at[target],
            recv_sem=rmsem.at[source],
            device_id=ident(target),
            device_id_type=pl.DeviceIdType.MESH,
        )

    def from_side(d, way):
        return z - d if way == RIGHT else z + d

    def side_exists(d, way):
        return z >= d if way == RIGHT else z < depth - d

    def main_step(d, k):
        for way in (LEFT, RIGHT):
            src = at(from_side(d, way), y, c)
            there = side_exists(d, way)

            @pl.when(there)
            def _():
                arrived(src, k)
                send(src, k, way, held=there)
                send(src, k, ACROSS, held=there)
                send(src, k, SIBLING, held=there)

    def side_step(d):
        for way in (LEFT, RIGHT):
            there = side_exists(d, way)

            pair = [at(from_side(d, way), line, c) for line in (y, yp)]

            @pl.when(there)
            def _():
                for src in pair:
                    arrived(src, last)
                    send(src, last, way, held=there)
                    send(src, last, SIBLING, held=there)

    def across_step(d):
        for k in range(last):
            if d == 0:
                src = at(z, yp, c)
                arrived(src, k)
                send(src, k, SIBLING)
                continue
            for way in (LEFT, RIGHT):
                src = at(from_side(d, way), yp, c)
                there = side_exists(d, way)

                @pl.when(there)
                def _():
                    arrived(src, k)
                    send(src, k, SIBLING, held=there)

    for d in range(1, depth):
        for k in range(last):
            main_step(d, k)
            if d == 1 and k == 0:
                for o in range(1, n):
                    note_of((me + o) % n, me).start()
        if d == 1:
            other = at(z, yp, c)
            arrived(other, last)
            send(other, last, SIBLING)
            for way in (LEFT, RIGHT):
                send(me, last, way, own=True)
                send(other, last, way)
        else:
            side_step(d - 1)
            if d == 2:
                across_step(0)
    across_step(1)
    side_step(depth - 1)
    for d in range(2, depth):
        across_step(d)

    for o in range(n // 2):
        src = at(o // 2, o % 2, cp)
        for k in range(last + 1):
            arrived(src, k)
    keep.wait()
    for held, way, src, k, own in sent:
        cond = exists[way]
        both = cond if held is None else held if cond is None else jnp.logical_and(held, cond)
        guarded(both, copy_of(src, k, way, own).wait_send)
    for o in range(1, n):
        note_of((me + o) % n, (me + n - o) % n).wait()


def expand_kernel(n, scale, tok_ref, rmsg, out_ref, loss_ref, select, gate):
    rows = tok_ref.shape[1]
    mine, slots, block = out_ref.shape
    windows = slots // 16
    step = pl.program_id(0)

    def sources(w):
        return 16 * w // CAP, min(n, (16 * w + 15) // CAP + 1)

    @pl.when(step == 0)
    def _():
        for w in range(windows):
            first, stop = sources(w)
            row = lax.broadcasted_iota(jnp.int32, (mine, 16, rows), 1).astype(jnp.float32)
            total = jnp.zeros((mine * 16, 1), jnp.float32)
            for s in range(first, stop):
                want = row + jnp.float32(16 * w - CAP * s)
                hit = jnp.logical_and(want >= 0.0, rmsg[s, 1][:, None, :] == want)
                at = (s - first) * rows
                one = jnp.where(hit, 1.0, 0.0).reshape(mine * 16, rows)
                select[w, :, at : at + rows] = one.astype(jnp.bfloat16)
                weight = jnp.where(hit, rmsg[s, 0][:, None, :], 0.0).reshape(mine * 16, rows)
                total = total + jnp.sum(weight, axis=1, keepdims=True)
            gate[w] = jnp.broadcast_to(total, (mine * 16, LANES))
        both = rmsg[0, 2]
        for s in range(1, n):
            both = both + rmsg[s, 2]
        loss = jnp.sum(both[0:1] * both[1:2], axis=1, keepdims=True) * scale
        loss_ref[...] = jnp.broadcast_to(loss, loss_ref.shape)

    cols = pl.ds(pl.multiple_of(step * block, block), block)
    for w in range(windows):
        first, stop = sources(w)
        depth = (stop - first) * rows
        tok = tok_ref[first:stop, :, cols].reshape(depth, block)
        got = jnp.dot(select[w, :, :depth], tok, preferred_element_type=jnp.float32)
        got = got * gate[w][:, 0:1]
        out_ref[:, 16 * w : 16 * w + 16, :] = got.astype(jnp.bfloat16).reshape(mine, 16, block)


def on_device_kernels(n, tokens, router_weight, expert_ids):
    rows, width = tokens.shape
    mine = EXPERTS // n
    chunks = len(column_chunks(width))
    vmem = pl.BlockSpec(memory_space=pltpu.VMEM)
    dma = pltpu.SemaphoreType.DMA
    gathered, notes = pl.pallas_call(
        functools.partial(gather_kernel, n),
        out_shape=(
            pltpu.VMEM((n, rows, width), jnp.bfloat16),
            pltpu.VMEM((n, 3, mine, EXPERTS), jnp.float32),
        ),
        in_specs=[vmem] * 3,
        out_specs=(vmem, vmem),
        scratch_shapes=[
            pltpu.VMEM((n, 3, mine, EXPERTS), jnp.float32),
            dma((n, chunks, 4)),
            dma((n, chunks)),
            dma((n,)),
            dma((n,)),
            dma(()),
        ],
        compiler_params=pltpu.CompilerParams(
            collective_id=0, has_side_effects=True, vmem_limit_bytes=30 * 2**20
        ),
    )(tokens, router_weight, expert_ids)
    total = rows * n
    scale = EXPERTS / (float(total) * total * TOP_K)
    block = 4 * LANES
    slots = n * CAP
    expert_rows, loss = pl.pallas_call(
        functools.partial(expand_kernel, n, scale),
        grid=(width // block,),
        out_shape=(
            jax.ShapeDtypeStruct((mine, slots, width), jnp.bfloat16),
            jax.ShapeDtypeStruct((8, LANES), jnp.float32),
        ),
        in_specs=[vmem] * 2,
        out_specs=(
            pl.BlockSpec((mine, slots, block), lambda i: (0, 0, i)),
            pl.BlockSpec((8, LANES), lambda i: (0, 0)),
        ),
        scratch_shapes=[
            pltpu.VMEM((slots // 16, mine * 16, 3 * rows), jnp.bfloat16),
            pltpu.VMEM((slots // 16, mine * 16, LANES), jnp.float32),
        ],
        compiler_params=pltpu.CompilerParams(vmem_limit_bytes=30 * 2**20),
    )(
        pltpu.with_memory_space_constraint(gathered, pltpu.VMEM),
        pltpu.with_memory_space_constraint(notes, pltpu.VMEM),
    )
    return expert_rows, loss[0, :1]


def on_device(tokens, router_weight, expert_ids):
    local_rows = tokens.shape[0]
    row_width = tokens.shape[1]
    logits = jnp.dot(tokens, router_weight, preferred_element_type=jnp.float32)
    probability = jax.nn.softmax(logits, axis=-1)
    gates = jax.nn.softmax(jnp.take_along_axis(logits, expert_ids, axis=1), axis=1)
    onehot = jnp.sum(
        (expert_ids[:, :, None] == jnp.arange(EXPERTS, dtype=jnp.int32)[None, None, :]).astype(
            jnp.int32
        ),
        axis=1,
    )
    before = jnp.cumsum(onehot, axis=0) - onehot
    slot_rank = jnp.take_along_axis(before, expert_ids, axis=1)
    slot_index = (expert_ids * CAP + slot_rank).reshape(-1)
    token_index = jnp.repeat(jnp.arange(local_rows, dtype=jnp.int32), TOP_K)
    slot_token = jnp.zeros((EXPERTS * CAP,), jnp.int32).at[slot_index].set(token_index)
    slot_gate = jnp.zeros((EXPERTS * CAP,), jnp.float32).at[slot_index].set(gates.reshape(-1))
    picked = tokens[slot_token]
    arrived = lax.all_to_all(
        picked.reshape(EXPERTS, CAP, row_width), "expert", split_axis=0, concat_axis=1, tiled=True
    )
    arrived_gates = lax.all_to_all(
        slot_gate.reshape(EXPERTS, CAP), "expert", split_axis=0, concat_axis=1, tiled=True
    )
    expert_rows = (arrived_gates[:, :, None] * arrived.astype(jnp.float32)).astype(jnp.bfloat16)
    expert_load = jnp.sum(onehot, axis=0).astype(jnp.float32)
    expert_mass = jnp.sum(probability, axis=0)
    token_total = jnp.float32(local_rows * lax.axis_size("expert"))
    load_all, mass_all = lax.psum((expert_load, expert_mass), "expert")
    summed = jnp.sum(load_all * mass_all)
    balance_loss = EXPERTS * summed / (token_total * token_total * TOP_K)
    return (expert_rows, balance_loss.reshape(1))


def solution(mesh):
    n = mesh.shape["expert"]

    def body(tokens, router_weight, expert_ids):
        rows, width = tokens.shape
        gathered = n * rows * width * 2
        fits = gathered <= 24 * 2**20 and (EXPERTS // n) % 8 == 0 and rows == EXPERTS
        if fits and n % 16 == 0 and width % 512 == 0:
            return on_device_kernels(n, tokens, router_weight, expert_ids)
        return on_device(tokens, router_weight, expert_ids)

    return jax.shard_map(
        body,
        mesh=mesh,
        in_specs=(P(("groups", "expert"), None), P(), P(("groups", "expert"), None)),
        out_specs=(P("expert", "groups", None), P("groups")),
        check_vma=False,
    )
```

```python
import functools

import jax
import jax.numpy as jnp
from jax import lax
from jax.experimental import pallas as pl
from jax.experimental.pallas import tpu as pltpu
from jax.sharding import PartitionSpec as P

EXPERTS = 128
TOP_K = 8
CAP = 9
LANES = 128
LEFT, RIGHT, ACROSS, SIBLING = range(4)
PIECES = 3


def column_chunks(width):
    tiles = width // LANES
    side = max(1, tiles * 5 // 32)
    main = tiles - side
    edges = [main * i // PIECES for i in range(PIECES + 1)] + [tiles]
    return [(a * LANES, (b - a) * LANES) for a, b in zip(edges[:-1], edges[1:])]


def dispatch_kernel(
    n, scale, x_hbm, w_hbm, ids_ref, out_ref, loss_ref,
    buf, w_ref, msg, notes, stat, stats, select, gate, ssem, rsem, nsem, tsem, lsem,
):
    depth = n // 4
    me = lax.axis_index("expert")
    group = lax.axis_index("groups")
    z, y, c = me // 4, (me // 2) % 2, me % 2
    yp, cp = 1 - y, 1 - c
    rows, width = x_hbm.shape
    mine, slots = out_ref.shape[:2]
    chunks = column_chunks(width)
    last = len(chunks) - 1
    span = chunks[0][1]

    def at(zz, yy, cc):
        return zz * 4 + yy * 2 + cc

    def ident(target):
        return (group, target)

    fetch = pltpu.make_async_copy(x_hbm, buf.at[me], lsem.at[0])
    fetch.start()
    fetch_w = pltpu.make_async_copy(w_hbm, w_ref, lsem.at[1])
    fetch_w.start()
    barrier = pltpu.get_barrier_semaphore()
    for o in range(1, n):
        pl.semaphore_signal(
            barrier, inc=1, device_id=ident((me + o) % n), device_id_type=pl.DeviceIdType.MESH
        )
    fetch.wait()
    pl.semaphore_wait(barrier, n - 1)

    where = {
        LEFT: at(z - 1, y, c),
        RIGHT: at(z + 1, y, c),
        ACROSS: at(z, yp, c),
        SIBLING: at(z, y, cp),
    }
    exists = {LEFT: z > 0, RIGHT: z < depth - 1, ACROSS: None, SIBLING: None}
    sent = []

    def copy_of(src, k, way):
        start, wide = chunks[k]
        part = buf.at[src, :, pl.ds(start, wide)]
        return pltpu.make_async_remote_copy(
            src_ref=part,
            dst_ref=part,
            send_sem=ssem.at[src, k, way],
            recv_sem=rsem.at[src, k],
            device_id=ident(where[way]),
            device_id_type=pl.DeviceIdType.MESH,
        )

    def guarded(cond, fn):
        if cond is None:
            fn()
        else:
            pl.when(cond)(fn)

    def send(src, k, way, held=None):
        guarded(exists[way], copy_of(src, k, way).start)
        sent.append((held, way, src, k))

    def arrived(src, k):
        copy_of(src, k, SIBLING).wait_recv()

    def own(k):
        for way in (LEFT, RIGHT, ACROSS, SIBLING):
            send(me, k, way)

    own(0)

    fetch_w.wait()
    logits = jnp.dot(buf[me], w_ref[...], preferred_element_type=jnp.float32)
    raised = jnp.exp(logits - jnp.max(logits, axis=1, keepdims=True))
    probability = raised / jnp.sum(raised, axis=1, keepdims=True)
    across = logits.T
    ids = ids_ref[...]
    expert = lax.broadcasted_iota(jnp.int32, (EXPERTS, rows), 0)
    named = ids[0:1, :] == expert
    for k in range(1, TOP_K):
        named = jnp.logical_or(named, ids[k : k + 1, :] == expert)
    mask = jnp.where(named, 1.0, 0.0)
    chosen = jnp.where(named, across, -1e30)
    picked = jnp.where(named, jnp.exp(chosen - jnp.max(chosen, axis=0, keepdims=True)), 0.0)
    gates = jnp.where(named, picked / jnp.sum(picked, axis=0, keepdims=True), -1.0)
    msg[...] = gates.reshape(n, mine, rows)
    stat[:, :EXPERTS] = jnp.sum(mask.T, axis=0, keepdims=True)
    stat[:, EXPERTS:] = jnp.sum(probability, axis=0, keepdims=True)
    notes[me] = msg[me]
    stats[me] = stat[...]

    @pl.loop(0, mine)
    def _(e):
        out_ref[e] = jnp.zeros(out_ref.shape[1:], out_ref.dtype)

    def note_of(target, source):
        return (
            pltpu.make_async_remote_copy(
                src_ref=msg.at[target],
                dst_ref=notes.at[source],
                send_sem=nsem.at[0, target],
                recv_sem=nsem.at[1, source],
                device_id=ident(target),
                device_id_type=pl.DeviceIdType.MESH,
            ),
            pltpu.make_async_remote_copy(
                src_ref=stat,
                dst_ref=stats.at[source],
                send_sem=tsem.at[0, target],
                recv_sem=tsem.at[1, source],
                device_id=ident(target),
                device_id_type=pl.DeviceIdType.MESH,
            ),
        )

    for o in range(1, n):
        for note in note_of((me + o) % n, me):
            note.start()
    for k in range(1, last):
        own(k)
    send(me, last, ACROSS)
    send(me, last, SIBLING)

    def from_side(d, way):
        return z - d if way == RIGHT else z + d

    def side_exists(d, way):
        return z >= d if way == RIGHT else z < depth - d

    def main_step(d, k):
        for way in (LEFT, RIGHT):
            src = at(from_side(d, way), y, c)
            there = side_exists(d, way)

            @pl.when(there)
            def _():
                arrived(src, k)
                send(src, k, way, held=there)
                send(src, k, ACROSS, held=there)
                send(src, k, SIBLING, held=there)

    def side_step(d):
        for way in (LEFT, RIGHT):
            there = side_exists(d, way)
            pair = [at(from_side(d, way), line, c) for line in (y, yp)]

            @pl.when(there)
            def _():
                for src in pair:
                    arrived(src, last)
                    send(src, last, way, held=there)
                    send(src, last, SIBLING, held=there)

    def across_step(d, k):
        if d == 0:
            src = at(z, yp, c)
            arrived(src, k)
            send(src, k, SIBLING)
            return
        for way in (LEFT, RIGHT):
            src = at(from_side(d, way), yp, c)
            there = side_exists(d, way)

            @pl.when(there)
            def _():
                arrived(src, k)
                send(src, k, SIBLING, held=there)

    def window(src):
        return jnp.minimum((CAP * src) // 16 * 16, slots - 32)

    def build(src):
        note = notes[src]
        chose = note >= 0.0
        r = lax.broadcasted_iota(jnp.int32, (rows, rows), 0)
        q = lax.broadcasted_iota(jnp.int32, (rows, rows), 1)
        upper = jnp.where(r < q, 1.0, 0.0).astype(jnp.bfloat16)
        ones = jnp.where(chose, 1.0, 0.0).astype(jnp.bfloat16)
        rank = jnp.dot(ones, upper, preferred_element_type=jnp.float32)
        rank = jnp.where(chose, rank, -100.0)
        row = lax.broadcasted_iota(jnp.int32, (mine, 32, rows), 1) + (window(src) - CAP * src)
        hit = row.astype(jnp.float32) == rank[:, None, :]
        one = jnp.where(hit, 1.0, 0.0).reshape(mine * 32, rows)
        select[src] = one.astype(jnp.bfloat16)
        weight = jnp.where(hit, note[:, None, :], 0.0).reshape(mine * 32, rows)
        total = jnp.sum(weight, axis=1, keepdims=True)
        gate[src] = jnp.broadcast_to(total, (mine * 32, LANES))

    def expand(src, start, wide):
        cols = pl.ds(start, wide)
        win = pl.ds(pl.multiple_of(window(src), 16), 32)
        got = jnp.dot(select[src], buf[src, :, cols], preferred_element_type=jnp.float32)
        got = (got * gate[src][:, 0:1]).astype(jnp.bfloat16).reshape(mine, 32, wide)
        out_ref[:, win, cols] = out_ref[:, win, cols] + got

    def from_sibling(src, k):
        pltpu.make_async_remote_copy(
            src_ref=part_of(src, k),
            dst_ref=part_of(src, k),
            send_sem=ssem.at[src, k, SIBLING],
            recv_sem=rsem.at[src, k],
            device_id=ident(where[SIBLING]),
            device_id_type=pl.DeviceIdType.MESH,
        ).wait_recv()

    def part_of(src, k):
        return buf.at[src, :, pl.ds(pl.multiple_of(k * span, LANES), span)]

    def fill_main(zs, line, first=0, stop=last):
        @pl.loop(0, 2 * (stop - first))
        def _(i):
            k = first + i // 2
            theirs = i % 2
            src = at(zs, line, jnp.where(theirs == 1, cp, c))

            @pl.when(theirs == 1)
            def _():
                from_sibling(src, k)

            expand(src, pl.multiple_of(k * span, LANES), span)

    def fill_side(zs):
        start, wide = chunks[last]

        @pl.loop(0, 4)
        def _(i):
            theirs = i % 2
            src = at(zs, i // 2, jnp.where(theirs == 1, cp, c))

            @pl.when(theirs == 1)
            def _():
                arrived(src, last)

            expand(src, start, wide)

    def fill_far(d, line, first=0, stop=last):
        @pl.loop(0, 2)
        def _(i):
            zs = jnp.where(i == 0, z - d, z + d)

            @pl.when(jnp.logical_and(zs >= 0, zs < depth))
            def _():
                fill_main(zs, line, first, stop)

    def fill_side_far(d):
        @pl.loop(0, 2)
        def _(i):
            zs = jnp.where(i == 0, z - d, z + d)

            @pl.when(jnp.logical_and(zs >= 0, zs < depth))
            def _():
                fill_side(zs)

    for d in range(1, depth):
        for k in range(last):
            main_step(d, k)
        if d == 1:
            other = at(z, yp, c)
            arrived(other, last)
            send(other, last, SIBLING)
            for way in (LEFT, RIGHT):
                send(me, last, way)
                send(other, last, way)
            for o in range(1, n):
                for note in note_of((me + o) % n, (me + n - o) % n):
                    note.wait()
            pl.loop(0, n)(build)
            fill_main(z, y)
            fill_side(z)
        else:
            side_step(d - 1)
            if d == 2:
                for k in range(last):
                    across_step(0, k)
                fill_far(1, y)
                fill_main(z, yp)
                fill_side_far(1)
    for d in range(2, depth):
        fill_far(d, y)
    for k in range(last):
        across_step(1, k)
    fill_far(1, yp)
    side_step(depth - 1)
    for d in range(2, depth):
        fill_side_far(d)
    both = jnp.sum(stats[...], axis=0)
    loss_ref[0] = jnp.sum(both[:, :EXPERTS] * both[:, EXPERTS:]) * scale
    for d in range(2, depth):
        for k in range(last):
            across_step(d, k)
            fill_far(d, yp, k, k + 1)

    for held, way, src, k in sent:
        cond = exists[way]
        both = cond if held is None else held if cond is None else jnp.logical_and(held, cond)
        guarded(both, copy_of(src, k, way).wait_send)


def on_device_kernels(n, tokens, router_weight, expert_ids):
    rows, width = tokens.shape
    mine = EXPERTS // n
    slots = n * CAP
    chunks = len(column_chunks(width))
    vmem = pl.BlockSpec(memory_space=pltpu.VMEM)
    hbm = pl.BlockSpec(memory_space=pltpu.HBM)
    dma = pltpu.SemaphoreType.DMA
    total = rows * n
    scale = EXPERTS / (float(total) * total * TOP_K)
    return pl.pallas_call(
        functools.partial(dispatch_kernel, n, scale),
        out_shape=(
            pltpu.VMEM((mine, slots, width), jnp.bfloat16),
            jax.ShapeDtypeStruct((1,), jnp.float32),
        ),
        in_specs=[hbm, hbm, vmem],
        out_specs=(vmem, pl.BlockSpec(memory_space=pltpu.SMEM)),
        scratch_shapes=[
            pltpu.VMEM((n, rows, width), jnp.bfloat16),
            pltpu.VMEM(router_weight.shape, jnp.bfloat16),
            pltpu.VMEM((n, mine, rows), jnp.float32),
            pltpu.VMEM((n, mine, rows), jnp.float32),
            pltpu.VMEM((1, 2 * EXPERTS), jnp.float32),
            pltpu.VMEM((n, 1, 2 * EXPERTS), jnp.float32),
            pltpu.VMEM((n, mine * 32, rows), jnp.bfloat16),
            pltpu.VMEM((n, mine * 32, LANES), jnp.float32),
            dma((n, chunks, 4)),
            dma((n, chunks)),
            dma((2, n)),
            dma((2, n)),
            dma((2,)),
        ],
        compiler_params=pltpu.CompilerParams(
            collective_id=0, has_side_effects=True, vmem_limit_bytes=40 * 2**20
        ),
    )(tokens, router_weight, expert_ids.T)


def on_device(tokens, router_weight, expert_ids):
    local_rows = tokens.shape[0]
    row_width = tokens.shape[1]
    logits = jnp.dot(tokens, router_weight, preferred_element_type=jnp.float32)
    probability = jax.nn.softmax(logits, axis=-1)
    gates = jax.nn.softmax(jnp.take_along_axis(logits, expert_ids, axis=1), axis=1)
    onehot = jnp.sum(
        (expert_ids[:, :, None] == jnp.arange(EXPERTS, dtype=jnp.int32)[None, None, :]).astype(
            jnp.int32
        ),
        axis=1,
    )
    before = jnp.cumsum(onehot, axis=0) - onehot
    slot_rank = jnp.take_along_axis(before, expert_ids, axis=1)
    slot_index = (expert_ids * CAP + slot_rank).reshape(-1)
    token_index = jnp.repeat(jnp.arange(local_rows, dtype=jnp.int32), TOP_K)
    slot_token = jnp.zeros((EXPERTS * CAP,), jnp.int32).at[slot_index].set(token_index)
    slot_gate = jnp.zeros((EXPERTS * CAP,), jnp.float32).at[slot_index].set(gates.reshape(-1))
    picked = tokens[slot_token]
    arrived = lax.all_to_all(
        picked.reshape(EXPERTS, CAP, row_width), "expert", split_axis=0, concat_axis=1, tiled=True
    )
    arrived_gates = lax.all_to_all(
        slot_gate.reshape(EXPERTS, CAP), "expert", split_axis=0, concat_axis=1, tiled=True
    )
    expert_rows = (arrived_gates[:, :, None] * arrived.astype(jnp.float32)).astype(jnp.bfloat16)
    expert_load = jnp.sum(onehot, axis=0).astype(jnp.float32)
    expert_mass = jnp.sum(probability, axis=0)
    token_total = jnp.float32(local_rows * lax.axis_size("expert"))
    load_all, mass_all = lax.psum((expert_load, expert_mass), "expert")
    summed = jnp.sum(load_all * mass_all)
    balance_loss = EXPERTS * summed / (token_total * token_total * TOP_K)
    return (expert_rows, balance_loss.reshape(1))


def solution(mesh):
    n = mesh.shape["expert"]

    def body(tokens, router_weight, expert_ids):
        rows, width = tokens.shape
        gathered = n * rows * width * 2
        fits = gathered <= 24 * 2**20 and (EXPERTS // n) % 8 == 0 and rows == EXPERTS
        if fits and n % 16 == 0 and width % (32 * LANES) == 0:
            return on_device_kernels(n, tokens, router_weight, expert_ids)
        return on_device(tokens, router_weight, expert_ids)

    return jax.shard_map(
        body,
        mesh=mesh,
        in_specs=(P(("groups", "expert"), None), P(), P(("groups", "expert"), None)),
        out_specs=(P("expert", "groups", None), P("groups")),
        check_vma=False,
    )
```

```python
import functools

import jax
import jax.numpy as jnp
from jax import lax
from jax.experimental import pallas as pl
from jax.experimental.pallas import tpu as pltpu
from jax.sharding import PartitionSpec as P

EXPERTS = 128
TOP_K = 8
CAP = 9
LANES = 128
LEFT, RIGHT, ACROSS, SIBLING = range(4)
PIECES = 3


def column_chunks(width):
    tiles = width // LANES
    side = max(1, tiles * 5 // 32)
    main = tiles - side
    edges = [main * i // PIECES for i in range(PIECES + 1)] + [tiles]
    return [(a * LANES, (b - a) * LANES) for a, b in zip(edges[:-1], edges[1:])]


def dispatch_kernel(
    n, scale, x_hbm, w_hbm, ids_ref, out_ref, loss_ref,
    buf, w_ref, msg, notes, stat, stats, select, gate, ssem, rsem, nsem, tsem, lsem,
):
    depth = n // 4
    me = lax.axis_index("expert")
    group = lax.axis_index("groups")
    z, y, c = me // 4, (me // 2) % 2, me % 2
    yp, cp = 1 - y, 1 - c
    rows, width = x_hbm.shape
    mine, slots = out_ref.shape[:2]
    chunks = column_chunks(width)
    last = len(chunks) - 1
    span = chunks[0][1]

    def at(zz, yy, cc):
        return zz * 4 + yy * 2 + cc

    def ident(target):
        return (group, target)

    fetch = pltpu.make_async_copy(x_hbm, buf.at[me], lsem.at[0])
    fetch.start()
    fetch_w = pltpu.make_async_copy(w_hbm, w_ref, lsem.at[1])
    fetch_w.start()
    barrier = pltpu.get_barrier_semaphore()
    for o in range(1, n):
        pl.semaphore_signal(
            barrier, inc=1, device_id=ident((me + o) % n), device_id_type=pl.DeviceIdType.MESH
        )
    fetch.wait()
    pl.semaphore_wait(barrier, n - 1)

    where = {
        LEFT: at(z - 1, y, c),
        RIGHT: at(z + 1, y, c),
        ACROSS: at(z, yp, c),
        SIBLING: at(z, y, cp),
    }
    exists = {LEFT: z > 0, RIGHT: z < depth - 1, ACROSS: None, SIBLING: None}
    sent = []

    def copy_of(src, k, way):
        start, wide = chunks[k]
        part = buf.at[src, :, pl.ds(start, wide)]
        return pltpu.make_async_remote_copy(
            src_ref=part,
            dst_ref=part,
            send_sem=ssem.at[src, k, way],
            recv_sem=rsem.at[src, k],
            device_id=ident(where[way]),
            device_id_type=pl.DeviceIdType.MESH,
        )

    def guarded(cond, fn):
        if cond is None:
            fn()
        else:
            pl.when(cond)(fn)

    def send(src, k, way, held=None):
        guarded(exists[way], copy_of(src, k, way).start)
        sent.append((held, way, src, k))

    def arrived(src, k):
        copy_of(src, k, SIBLING).wait_recv()

    def own(k):
        for way in (LEFT, RIGHT, ACROSS, SIBLING):
            send(me, k, way)

    own(0)

    fetch_w.wait()
    logits = jnp.dot(buf[me], w_ref[...], preferred_element_type=jnp.float32)
    raised = jnp.exp(logits - jnp.max(logits, axis=1, keepdims=True))
    probability = raised / jnp.sum(raised, axis=1, keepdims=True)
    across = logits.T
    ids = ids_ref[...]
    expert = lax.broadcasted_iota(jnp.int32, (EXPERTS, rows), 0)
    named = ids[0:1, :] == expert
    for k in range(1, TOP_K):
        named = jnp.logical_or(named, ids[k : k + 1, :] == expert)
    mask = jnp.where(named, 1.0, 0.0)
    chosen = jnp.where(named, across, -1e30)
    picked = jnp.where(named, jnp.exp(chosen - jnp.max(chosen, axis=0, keepdims=True)), 0.0)
    gates = jnp.where(named, picked / jnp.sum(picked, axis=0, keepdims=True), -1.0)
    msg[...] = gates.reshape(n, mine, rows)
    stat[:, :EXPERTS] = jnp.sum(mask.T, axis=0, keepdims=True)
    stat[:, EXPERTS:] = jnp.sum(probability, axis=0, keepdims=True)
    notes[me] = msg[me]
    stats[me] = stat[...]

    @pl.loop(0, mine)
    def _(e):
        out_ref[e] = jnp.zeros(out_ref.shape[1:], out_ref.dtype)

    def note_of(target, source):
        return (
            pltpu.make_async_remote_copy(
                src_ref=msg.at[target],
                dst_ref=notes.at[source],
                send_sem=nsem.at[0, target],
                recv_sem=nsem.at[1, source],
                device_id=ident(target),
                device_id_type=pl.DeviceIdType.MESH,
            ),
            pltpu.make_async_remote_copy(
                src_ref=stat,
                dst_ref=stats.at[source],
                send_sem=tsem.at[0, target],
                recv_sem=tsem.at[1, source],
                device_id=ident(target),
                device_id_type=pl.DeviceIdType.MESH,
            ),
        )

    for o in range(1, n):
        for note in note_of((me + o) % n, me):
            note.start()
    for k in range(1, last):
        own(k)
    send(me, last, ACROSS)
    send(me, last, SIBLING)

    def from_side(d, way):
        return z - d if way == RIGHT else z + d

    def side_exists(d, way):
        return z >= d if way == RIGHT else z < depth - d

    def main_step(d, k):
        for way in (LEFT, RIGHT):
            src = at(from_side(d, way), y, c)
            there = side_exists(d, way)

            @pl.when(there)
            def _():
                arrived(src, k)
                send(src, k, way, held=there)
                send(src, k, ACROSS, held=there)
                send(src, k, SIBLING, held=there)

    def side_step(d):
        for way in (LEFT, RIGHT):
            there = side_exists(d, way)
            pair = [at(from_side(d, way), line, c) for line in (y, yp)]

            @pl.when(there)
            def _():
                for src in pair:
                    arrived(src, last)
                    send(src, last, way, held=there)
                    send(src, last, SIBLING, held=there)

    def across_step(d, k):
        if d == 0:
            src = at(z, yp, c)
            arrived(src, k)
            send(src, k, SIBLING)
            return
        for way in (LEFT, RIGHT):
            src = at(from_side(d, way), yp, c)
            there = side_exists(d, way)

            @pl.when(there)
            def _():
                arrived(src, k)
                send(src, k, SIBLING, held=there)

    def window(chip):
        return jnp.minimum((2 * CAP * chip) // 16 * 16, slots - 32)

    def build(chip):
        r = lax.broadcasted_iota(jnp.int32, (rows, rows), 0)
        q = lax.broadcasted_iota(jnp.int32, (rows, rows), 1)
        upper = jnp.where(r < q, 1.0, 0.0).astype(jnp.bfloat16)
        total = jnp.zeros((mine * 32, 1), jnp.float32)
        for core in range(2):
            src = 2 * chip + core
            note = notes[src]
            chose = note >= 0.0
            ones = jnp.where(chose, 1.0, 0.0).astype(jnp.bfloat16)
            rank = jnp.dot(ones, upper, preferred_element_type=jnp.float32)
            rank = jnp.where(chose, rank, -100.0)
            row = lax.broadcasted_iota(jnp.int32, (mine, 32, rows), 1) + (window(chip) - CAP * src)
            hit = row.astype(jnp.float32) == rank[:, None, :]
            one = jnp.where(hit, 1.0, 0.0).reshape(mine * 32, rows)
            select[chip, :, core * rows : (core + 1) * rows] = one.astype(jnp.bfloat16)
            weight = jnp.where(hit, note[:, None, :], 0.0).reshape(mine * 32, rows)
            total = total + jnp.sum(weight, axis=1, keepdims=True)
        gate[chip] = jnp.broadcast_to(total, (mine * 32, LANES))

    def expand(chip, start, wide):
        cols = pl.ds(start, wide)
        win = pl.ds(pl.multiple_of(window(chip), 16), 32)
        tok = buf[pl.ds(2 * chip, 2), :, cols].reshape(2 * rows, wide)
        got = jnp.dot(select[chip], tok, preferred_element_type=jnp.float32)
        got = (got * gate[chip][:, 0:1]).astype(jnp.bfloat16).reshape(mine, 32, wide)
        out_ref[:, win, cols] = out_ref[:, win, cols] + got

    def from_sibling(src, k):
        pltpu.make_async_remote_copy(
            src_ref=part_of(src, k),
            dst_ref=part_of(src, k),
            send_sem=ssem.at[src, k, SIBLING],
            recv_sem=rsem.at[src, k],
            device_id=ident(where[SIBLING]),
            device_id_type=pl.DeviceIdType.MESH,
        ).wait_recv()

    def part_of(src, k):
        return buf.at[src, :, pl.ds(pl.multiple_of(k * span, LANES), span)]

    def fill_main(zs, line, first=0, stop=last):
        @pl.loop(first, stop)
        def _(k):
            from_sibling(at(zs, line, cp), k)
            expand(zs * 2 + line, pl.multiple_of(k * span, LANES), span)

    def fill_side(zs):
        @pl.loop(0, 2)
        def _(line):
            arrived(at(zs, line, cp), last)
            expand(zs * 2 + line, *chunks[last])

    def fill_far(d, line, first=0, stop=last):
        @pl.loop(0, 2)
        def _(i):
            zs = jnp.where(i == 0, z - d, z + d)

            @pl.when(jnp.logical_and(zs >= 0, zs < depth))
            def _():
                fill_main(zs, line, first, stop)

    def fill_side_far(d):
        @pl.loop(0, 2)
        def _(i):
            zs = jnp.where(i == 0, z - d, z + d)

            @pl.when(jnp.logical_and(zs >= 0, zs < depth))
            def _():
                fill_side(zs)

    for d in range(1, depth):
        for k in range(last):
            main_step(d, k)
            if d == 2:
                fill_main(z, y, k, k + 1)
            if d == 3:
                fill_main(z, yp, k, k + 1)
                fill_far(1, y, k, k + 1)
                fill_far(2, y, k, k + 1)
        if d == 1:
            other = at(z, yp, c)
            arrived(other, last)
            send(other, last, SIBLING)
            for way in (LEFT, RIGHT):
                send(me, last, way)
                send(other, last, way)
            for o in range(1, n):
                for note in note_of((me + o) % n, (me + n - o) % n):
                    note.wait()
            pl.loop(0, n // 2)(build)
            both = jnp.sum(stats[...], axis=0)
            loss_ref[0] = jnp.sum(both[:, :EXPERTS] * both[:, EXPERTS:]) * scale
        else:
            side_step(d - 1)
            if d == 2:
                fill_side(z)
                for k in range(last):
                    across_step(0, k)
    for k in range(last):
        across_step(1, k)
    fill_far(1, yp)
    fill_side_far(1)
    side_step(depth - 1)
    for d in range(3, depth):
        fill_far(d, y)
    for d in range(2, depth):
        fill_side_far(d)
    for d in range(2, depth):
        for k in range(last):
            across_step(d, k)
            fill_far(d, yp, k, k + 1)

    for held, way, src, k in sent:
        cond = exists[way]
        both = cond if held is None else held if cond is None else jnp.logical_and(held, cond)
        guarded(both, copy_of(src, k, way).wait_send)


def on_device_kernels(n, tokens, router_weight, expert_ids):
    rows, width = tokens.shape
    mine = EXPERTS // n
    slots = n * CAP
    chunks = len(column_chunks(width))
    vmem = pl.BlockSpec(memory_space=pltpu.VMEM)
    hbm = pl.BlockSpec(memory_space=pltpu.HBM)
    dma = pltpu.SemaphoreType.DMA
    total = rows * n
    scale = EXPERTS / (float(total) * total * TOP_K)
    return pl.pallas_call(
        functools.partial(dispatch_kernel, n, scale),
        out_shape=(
            pltpu.VMEM((mine, slots, width), jnp.bfloat16),
            jax.ShapeDtypeStruct((1,), jnp.float32),
        ),
        in_specs=[hbm, hbm, vmem],
        out_specs=(vmem, pl.BlockSpec(memory_space=pltpu.SMEM)),
        scratch_shapes=[
            pltpu.VMEM((n, rows, width), jnp.bfloat16),
            pltpu.VMEM(router_weight.shape, jnp.bfloat16),
            pltpu.VMEM((n, mine, rows), jnp.float32),
            pltpu.VMEM((n, mine, rows), jnp.float32),
            pltpu.VMEM((1, 2 * EXPERTS), jnp.float32),
            pltpu.VMEM((n, 1, 2 * EXPERTS), jnp.float32),
            pltpu.VMEM((n // 2, mine * 32, 2 * rows), jnp.bfloat16),
            pltpu.VMEM((n // 2, mine * 32, LANES), jnp.float32),
            dma((n, chunks, 4)),
            dma((n, chunks)),
            dma((2, n)),
            dma((2, n)),
            dma((2,)),
        ],
        compiler_params=pltpu.CompilerParams(
            collective_id=0, has_side_effects=True, vmem_limit_bytes=54 * 2**20 + 2**19
        ),
    )(tokens, router_weight, expert_ids.T)


def on_device(tokens, router_weight, expert_ids):
    local_rows = tokens.shape[0]
    row_width = tokens.shape[1]
    logits = jnp.dot(tokens, router_weight, preferred_element_type=jnp.float32)
    probability = jax.nn.softmax(logits, axis=-1)
    gates = jax.nn.softmax(jnp.take_along_axis(logits, expert_ids, axis=1), axis=1)
    onehot = jnp.sum(
        (expert_ids[:, :, None] == jnp.arange(EXPERTS, dtype=jnp.int32)[None, None, :]).astype(
            jnp.int32
        ),
        axis=1,
    )
    before = jnp.cumsum(onehot, axis=0) - onehot
    slot_rank = jnp.take_along_axis(before, expert_ids, axis=1)
    slot_index = (expert_ids * CAP + slot_rank).reshape(-1)
    token_index = jnp.repeat(jnp.arange(local_rows, dtype=jnp.int32), TOP_K)
    slot_token = jnp.zeros((EXPERTS * CAP,), jnp.int32).at[slot_index].set(token_index)
    slot_gate = jnp.zeros((EXPERTS * CAP,), jnp.float32).at[slot_index].set(gates.reshape(-1))
    picked = tokens[slot_token]
    arrived = lax.all_to_all(
        picked.reshape(EXPERTS, CAP, row_width), "expert", split_axis=0, concat_axis=1, tiled=True
    )
    arrived_gates = lax.all_to_all(
        slot_gate.reshape(EXPERTS, CAP), "expert", split_axis=0, concat_axis=1, tiled=True
    )
    expert_rows = (arrived_gates[:, :, None] * arrived.astype(jnp.float32)).astype(jnp.bfloat16)
    expert_load = jnp.sum(onehot, axis=0).astype(jnp.float32)
    expert_mass = jnp.sum(probability, axis=0)
    token_total = jnp.float32(local_rows * lax.axis_size("expert"))
    load_all, mass_all = lax.psum((expert_load, expert_mass), "expert")
    summed = jnp.sum(load_all * mass_all)
    balance_loss = EXPERTS * summed / (token_total * token_total * TOP_K)
    return (expert_rows, balance_loss.reshape(1))


def solution(mesh):
    n = mesh.shape["expert"]

    def body(tokens, router_weight, expert_ids):
        rows, width = tokens.shape
        gathered = n * rows * width * 2
        fits = gathered <= 24 * 2**20 and (EXPERTS // n) % 8 == 0 and rows == EXPERTS
        if fits and n == 16 and width % (32 * LANES) == 0:
            return on_device_kernels(n, tokens, router_weight, expert_ids)
        return on_device(tokens, router_weight, expert_ids)

    return jax.shard_map(
        body,
        mesh=mesh,
        in_specs=(P(("groups", "expert"), None), P(), P(("groups", "expert"), None)),
        out_specs=(P("expert", "groups", None), P("groups")),
        check_vma=False,
    )
```
